32 devices in a mesh: dp: 1 (over z), pz: 4 (over y), py: 4 (over x), px: 2 (over core).
Axes of the slice: x: 4, y: 4, z: 1, core: 2. Of those that a mesh axis runs over, the one named last changes fastest.
The devices are a block of a 4x4x8 slice.
Arguments:
- volumes: bfloat16 [2, 16, 64, 128, 128], P('dp', None, 'px', 'py', 'pz')
- filter_taps: float32 [3, 3, 17], replicated
- mix_weight: bfloat16 [3, 16, 16], replicated
- mix_bias: float32 [3, 16], replicated
Outputs:
- output: bfloat16 [2, 16, 64, 128, 128], P('dp', None, 'px', 'py', 'pz')
All inputs are finite; a program needn't handle non-finite values.
Results may differ from the reference program's by a relative error of at most 0.00376.
Values are sent between devices in bfloat16 or wider.
A program may use at most 768 MiB of HBM per device.

```python
import jax
import jax.numpy as jnp
from jax import lax

CHANNELS = 16
TAPS = 17
LAYERS = 3
VOLUMES = 2
EXTENT_X = 64
EXTENT_Y = 128
EXTENT_Z = 128
HALF_WIDTH = (TAPS - 1) // 2


def setup_inputs(seed: int = 0, part: int = 0) -> dict:
    root_key = jax.random.key(seed)
    key_vol, key_sign, key_mag, key_mix, key_bias = jax.random.split(root_key, 5)
    vol_key = jax.random.fold_in(key_vol, part)
    volumes = jax.random.normal(vol_key, (VOLUMES, CHANNELS, EXTENT_X, EXTENT_Y, EXTENT_Z), jnp.float32).astype(jnp.bfloat16)
    tap_signs = jax.random.bernoulli(key_sign, 0.5, (LAYERS, 3, TAPS)).astype(jnp.float32) * 2.0 - 1.0
    tap_sizes = jax.random.uniform(key_mag, (LAYERS, 3, TAPS), jnp.float32, 0.5, 1.5)
    raw_taps = tap_signs * tap_sizes
    filter_taps = raw_taps / jnp.sqrt(jnp.sum(raw_taps * raw_taps, axis=-1, keepdims=True))
    mix_weight = (jax.random.normal(key_mix, (LAYERS, CHANNELS, CHANNELS), jnp.float32) * CHANNELS ** -0.5).astype(jnp.bfloat16)
    mix_bias = 0.5 * jax.random.normal(key_bias, (LAYERS, CHANNELS), jnp.float32)
    return {'volumes': volumes, 'filter_taps': filter_taps, 'mix_weight': mix_weight, 'mix_bias': mix_bias}


def line_filter(field_3d, tap_row, axis_dim):
    extent = field_3d.shape[axis_dim]
    pad_spec = [(0, 0), (0, 0), (0, 0)]
    pad_spec[axis_dim] = (HALF_WIDTH, HALF_WIDTH)
    padded = jnp.pad(field_3d.astype(jnp.float32), pad_spec)
    taps_used = tap_row.astype(jnp.bfloat16).astype(jnp.float32)
    acc_sum = jnp.zeros(field_3d.shape, jnp.float32)
    for offset in range(TAPS):
        acc_sum = acc_sum + taps_used[offset] * lax.slice_in_dim(padded, offset, offset + extent, axis=axis_dim)
    return acc_sum.astype(jnp.bfloat16)


def layer_step(vol_state, layer_params):
    tap_block, weight, bias_row = layer_params

    def one_volume(volume):
        def one_channel(field_3d):
            field_3d = line_filter(field_3d, tap_block[0], 0)
            field_3d = line_filter(field_3d, tap_block[1], 1)
            return line_filter(field_3d, tap_block[2], 2)

        filtered = lax.map(one_channel, volume)
        flat_units = filtered.reshape(CHANNELS, -1)
        mix_out = jnp.dot(weight.T, flat_units, preferred_element_type=jnp.float32).reshape(volume.shape)
        activated = jax.nn.gelu(mix_out + bias_row[:, None, None, None], approximate=True)
        return (volume.astype(jnp.float32) + activated).astype(jnp.bfloat16)

    return lax.map(one_volume, vol_state), None


def reference(volumes, filter_taps, mix_weight, mix_bias):
    outcome = lax.scan(layer_step, volumes, (filter_taps, mix_weight, mix_bias))
    return outcome[0]
```

```python
import functools
import math

import jax
import jax.numpy as jnp
from jax import lax
from jax.experimental import pallas as pl
from jax.experimental.pallas import tpu as pltpu
from jax.sharding import PartitionSpec as P

MESH = pl.DeviceIdType.MESH
F32 = jnp.float32
BF16 = jnp.bfloat16
LAG_B = 3
LAG_C = 6


def dot(a, b):
    return jnp.dot(a, b, preferred_element_type=F32)


def iota2(shape, dim):
    return lax.broadcasted_iota(jnp.int32, shape, dim)


def kernel(cfg, x_hbm, taps, wt, bias, out_hbm, stage, vb, u1, u2, ob, jsend, jlo, jhi, ksend, klo, khi,
           mi, mj, mjh, mk, mkh, mw, ms, bcol, in_sem, out_sem, xs_sem, xr_sem, js_sem, jr_sem, ks_sem, kr_sem):
    layers, vols, nq, chans, ext, h, ktaps, ny, nz = cfg
    per_layer = vols * nq
    total = layers * per_layer
    px, py, pz = lax.axis_index("px"), lax.axis_index("py"), lax.axis_index("pz")
    mate = 1 - px
    y_lo, y_hi, z_lo, z_hi = py > 0, py < ny - 1, pz > 0, pz < nz - 1

    def place(q):
        return px * q + (1 - px) * (nq - 1 - q)

    def in_copy(c):
        v, q = c // nq, c % nq
        return pltpu.make_async_copy(x_hbm.at[v, :, pl.ds(place(q) * h, h)], stage.at[c], in_sem.at[c])

    for c in range(per_layer):
        in_copy(c).start()

    barrier = pltpu.get_barrier_semaphore()
    pl.semaphore_signal(barrier, inc=1, device_id={"px": mate}, device_id_type=MESH)
    for cond, name, other in ((y_lo, "py", py - 1), (y_hi, "py", py + 1), (z_lo, "pz", pz - 1), (z_hi, "pz", pz + 1)):
        @pl.when(cond)
        def _(name=name, other=other):
            pl.semaphore_signal(barrier, inc=1, device_id={name: other}, device_id_type=MESH)

    lanes = iota2((ext, 256), 1)
    rows = iota2((ext, 256), 0)

    def banded(layer, axis, diff):
        acc = jnp.zeros(diff.shape, F32)
        base = (layer * 3 + axis) * ktaps
        for t in range(ktaps):
            acc = jnp.where(diff == t, taps[base + t], acc)
        return acc

    for q in range(2):
        dirn, hh, i8, kk = lanes // 128, (lanes // 64) % 2, (lanes // h) % 8, lanes % h
        for g in range(8):
            hit = (hh == q) & (i8 == g) & (rows == kk + (ext - h) * dirn)
            ms[q, pl.ds(g * ext, ext), :] = jnp.where(hit, 1.0, 0.0).astype(BF16)

    def build(layer, _):
        lane_i, lane_k = lanes // ext, lanes % ext
        for i_in in range(3 * h):
            val = banded(layer, 0, i_in - lane_i[:8, :])
            full = jnp.concatenate([val] * (ext // 8), axis=0)
            mi[layer, pl.ds(i_in * ext, ext), :] = jnp.where(lane_k == rows, full, 0.0).astype(BF16)
        tj = banded(layer, 1, lane_k - rows + h)
        tk = banded(layer, 2, rows - lane_k + h)
        for g in range(8):
            mj[layer, pl.ds(g * ext, ext), :] = jnp.where(lane_i == g, tj, 0.0).astype(BF16)
            mk[layer, pl.ds(g * ext, ext), :] = jnp.where(lane_i == g, tk, 0.0).astype(BF16)
        l2, r2 = lanes[:, :128], rows[:, :128]
        d2, c2, jj = l2 // 64, (l2 // h) % 8, l2 % h
        tjh = banded(layer, 1, jj + d2 * (ext + h) - r2)
        for g in range(8):
            mjh[layer, pl.ds(g * ext, ext), :] = jnp.where(c2 == g, tjh, 0.0).astype(BF16)
        l3, r3 = lanes[:16, :], rows[:16, :]
        zero = jnp.zeros((64, 256), BF16)
        for d in range(2):
            tkh = banded(layer, 2, r3 % h + d * (ext + h) - l3 % ext)
            for half in range(2):
                mkh[layer, 1 - half, pl.ds(d * 128 + half * 64, 64), :] = zero
                for g in range(0, 8, 2):
                    part = jnp.where(l3 // ext == g + r3 // h, tkh, 0.0).astype(BF16)
                    mkh[layer, half, pl.ds(d * 128 + half * 64 + g * h, 16), :] = part
        r4, l4 = iota2((256, 16), 0), iota2((256, 16), 1)
        e_rows = jnp.where(r4 // 16 == l4, 1.0, 0.0).astype(BF16)
        r5, l5 = iota2((16, 256), 0), iota2((16, 256), 1)
        e_cols = jnp.where(l5 // 16 == r5, 1.0, 0.0).astype(BF16)
        wide = dot(dot(e_rows, wt[layer]).astype(BF16), e_cols)
        rw, lw = iota2((256, 256), 0), iota2((256, 256), 1)
        mw[layer] = jnp.where(rw % 16 == lw % 16, wide, 0.0).astype(BF16)
        bcol[layer] = jnp.broadcast_to(bias[layer], (256, 128))
        return 0

    lax.fori_loop(0, layers, build, 0)

    edge_slot = (1 - px) * 0 + px * (nq + 1)
    big_zero = jnp.zeros((512, 256), BF16)
    for l in range(layers):
        for v in range(vols):
            vb[l, v, edge_slot] = big_zero
    jlo[total] = jnp.zeros((128, 256), BF16)
    jhi[total] = jnp.zeros((128, 256), BF16)
    klo[total] = jnp.zeros((256, 128), BF16)
    khi[total] = jnp.zeros((256, 128), BF16)

    n_wait = 1 + (py > 0).astype(jnp.int32) + (py < ny - 1).astype(jnp.int32) + (pz > 0).astype(jnp.int32) + (pz < nz - 1).astype(jnp.int32)
    pl.semaphore_wait(barrier, n_wait)

    def x_copy(l, v):
        src = px * 1 + (1 - px) * nq
        dst = px * (nq + 1)
        return pltpu.make_async_remote_copy(vb.at[l, v, src], vb.at[l, v, dst], xs_sem.at[l, v], xr_sem.at[l, v],
                                            device_id={"px": mate}, device_id_type=MESH)

    def j_copies(n):
        return (
            (y_hi, y_lo, pltpu.make_async_remote_copy(jsend.at[n, 1], jlo.at[n], js_sem.at[n, 1], jr_sem.at[n, 0],
                                                      device_id={"py": py + 1}, device_id_type=MESH)),
            (y_lo, y_hi, pltpu.make_async_remote_copy(jsend.at[n, 0], jhi.at[n], js_sem.at[n, 0], jr_sem.at[n, 1],
                                                      device_id={"py": py - 1}, device_id_type=MESH)),
        )

    def k_copies(n):
        return (
            (z_hi, z_lo, pltpu.make_async_remote_copy(ksend.at[n, 1], klo.at[n], ks_sem.at[n, 1], kr_sem.at[n, 0],
                                                      device_id={"pz": pz + 1}, device_id_type=MESH)),
            (z_lo, z_hi, pltpu.make_async_remote_copy(ksend.at[n, 0], khi.at[n], ks_sem.at[n, 0], kr_sem.at[n, 1],
                                                      device_id={"pz": pz - 1}, device_id_type=MESH)),
        )

    def convert(c):
        v, q = c // nq, c % nq
        in_copy(c).wait()
        parts = [stage[c, :, a].reshape(chans * ext, ext) for a in range(h)]
        vb[0, v, place(q) + 1] = jnp.concatenate(parts, axis=1)

        @pl.when(q == 0)
        def _():
            x_copy(0, v).start()

    def index(n):
        return n // per_layer, (n // nq) % vols, n % nq

    def stage_a(n):
        l, v, q = index(n)

        @pl.when(q == 0)
        def _():
            x_copy(l, v).wait_recv()

        s = place(q) + 1
        acc = dot(vb[l, v, s - 1], mi[l, 0:256]) + dot(vb[l, v, s], mi[l, 256:512]) + dot(vb[l, v, s + 1], mi[l, 512:768])
        u1[n % 8] = acc.astype(BF16)
        cut = acc.reshape(chans, ext // h, h, 256)
        jsend[n, 0] = cut[:, 0].reshape(chans * h, 256).astype(BF16)
        jsend[n, 1] = cut[:, ext // h - 1].reshape(chans * h, 256).astype(BF16)
        for there, _, copy in j_copies(n):
            pl.when(there)(copy.start)

    def stage_b(n):
        l, v, q = index(n)
        for _, here, copy in j_copies(n):
            pl.when(here)(copy.wait_recv)
        n_lo = jnp.where(y_lo, n, total)
        n_hi = jnp.where(y_hi, n, total)
        packed = None
        for half in range(2):
            main = u1[n % 8, pl.ds(half * 256, 256), :]
            halo = jnp.concatenate([jlo[n_lo, pl.ds(half * 64, 64), :], jhi[n_hi, pl.ds(half * 64, 64), :]], axis=0)
            acc = (dot(mj[l], main) + dot(mjh[l], halo)).astype(BF16)
            u2[n % 8, pl.ds(half * 256, 256), :] = acc
            term = dot(acc, ms[half])
            packed = term if packed is None else packed + term
        packed = packed.astype(BF16)
        ksend[n, 0] = packed[:, :128]
        ksend[n, 1] = packed[:, 128:]
        for there, _, copy in k_copies(n):
            pl.when(there)(copy.start)

    def stage_c(n):
        l, v, q = index(n)
        for _, here, copy in k_copies(n):
            pl.when(here)(copy.wait_recv)
        n_lo = jnp.where(z_lo, n, total)
        n_hi = jnp.where(z_hi, n, total)
        halo = jnp.concatenate([klo[n_lo], khi[n_hi]], axis=1)
        u3 = []
        for half in range(2):
            acc = dot(u2[n % 8, pl.ds(half * 256, 256), :], mk[l]) + dot(halo, mkh[l, half])
            u3.append(acc.astype(BF16).reshape(8, 2, 16, 256))
        s = place(q) + 1
        old = vb[l, v, s].reshape(chans, 2, 16, 256)
        b128 = bcol[l]
        shift = jnp.concatenate([b128, b128], axis=1)
        new = []
        for jh in range(2):
            rhs = jnp.concatenate([u3[0][:, jh].reshape(128, 256), u3[1][:, jh].reshape(128, 256)], axis=0)
            z = dot(mw[l], rhs) + shift
            inner = z * (math.sqrt(2.0 / math.pi) + (0.044715 * math.sqrt(2.0 / math.pi)) * (z * z))
            half_z = 0.5 * z
            act = half_z + half_z * jnp.tanh(inner)
            res = old[:, jh].reshape(256, 256).astype(F32) + act
            new.append(res.astype(BF16).reshape(chans, 1, 16, 256))
        result = jnp.concatenate(new, axis=1).reshape(512, 256)

        @pl.when(l < layers - 1)
        def _():
            vb[l + 1, v, s] = result

            @pl.when(q == 0)
            def _():
                x_copy(l + 1, v).start()

        @pl.when(l == layers - 1)
        def _():
            c = v * nq + q
            ob[c] = result
            out_copy(v, q).start()

    def out_copy(v, q):
        c = v * nq + q
        return pltpu.make_async_copy(ob.at[c], out_hbm.at[v, place(q)], out_sem.at[c])

    convert(0)
    convert(1)

    def tick(t, _):
        @pl.when(t + 2 < per_layer)
        def _():
            convert(t + 2)

        @pl.when(t >= LAG_C)
        def _():
            stage_c(t - LAG_C)

        @pl.when((t >= LAG_B) & (t < total + LAG_B))
        def _():
            stage_b(t - LAG_B)

        @pl.when(t < total)
        def _():
            stage_a(t)
        return 0

    lax.fori_loop(0, total + LAG_C, tick, 0)

    def drain(n, _):
        for there, _, copy in j_copies(n) + k_copies(n):
            pl.when(there)(copy.wait_send)
        return 0

    lax.fori_loop(0, total, drain, 0)
    for l in range(layers):
        for v in range(vols):
            x_copy(l, v).wait_send()
    for v in range(vols):
        for q in range(nq):
            out_copy(v, q).wait()


def unpack_kernel(x_ref, o_ref):
    chans, h, ext = o_ref.shape[1:4]
    for a in range(h):
        o_ref[0, :, a] = x_ref[0, 0, :, a * ext:(a + 1) * ext].reshape(chans, ext, ext)


def solution(mesh):
    ny, nz = mesh.shape["py"], mesh.shape["pz"]
    spec = P("dp", None, "px", "py", "pz")

    def local(x, filter_taps, mix_weight, mix_bias):
        vols, chans, ext = x.shape[0], x.shape[1], x.shape[2]
        layers, ktaps = filter_taps.shape[0], filter_taps.shape[2]
        h = (ktaps - 1) // 2
        nq = ext // h
        total = layers * vols * nq
        cfg = (layers, vols, nq, chans, ext, h, ktaps, ny, nz)
        wt = jnp.swapaxes(mix_weight, 1, 2)
        bias = jnp.repeat(mix_bias, 16, axis=1)[:, :, None]
        vmem = functools.partial(pltpu.VMEM, dtype=BF16)
        dense = pl.pallas_call(
            functools.partial(kernel, cfg),
            out_shape=jax.ShapeDtypeStruct((vols, nq, 512, 256), BF16),
            in_specs=[
                pl.BlockSpec(memory_space=pl.ANY),
                pl.BlockSpec(memory_space=pltpu.SMEM),
                pl.BlockSpec(memory_space=pltpu.VMEM),
                pl.BlockSpec(memory_space=pltpu.VMEM),
            ],
            out_specs=pl.BlockSpec(memory_space=pl.ANY),
            scratch_shapes=[
                pltpu.VMEM((vols * nq, chans, h, ext, ext), BF16),
                pltpu.VMEM((layers, vols, nq + 2, 512, 256), BF16),
                pltpu.VMEM((8, 512, 256), BF16),
                pltpu.VMEM((8, 512, 256), BF16),
                pltpu.VMEM((vols * nq, 512, 256), BF16),
                pltpu.VMEM((total, 2, 128, 256), BF16),
                pltpu.VMEM((total + 1, 128, 256), BF16),
                pltpu.VMEM((total + 1, 128, 256), BF16),
                pltpu.VMEM((total, 2, 256, 128), BF16),
                pltpu.VMEM((total + 1, 256, 128), BF16),
                pltpu.VMEM((total + 1, 256, 128), BF16),
                pltpu.VMEM((layers, 768, 256), BF16),
                pltpu.VMEM((layers, 256, 256), BF16),
                pltpu.VMEM((layers, 256, 128), BF16),
                pltpu.VMEM((layers, 256, 256), BF16),
                pltpu.VMEM((layers, 2, 256, 256), BF16),
                pltpu.VMEM((layers, 256, 256), BF16),
                pltpu.VMEM((2, 256, 256), BF16),
                pltpu.VMEM((layers, 256, 128), F32),
                pltpu.SemaphoreType.DMA((vols * nq,)),
                pltpu.SemaphoreType.DMA((vols * nq,)),
                pltpu.SemaphoreType.DMA((layers, vols)),
                pltpu.SemaphoreType.DMA((layers, vols)),
                pltpu.SemaphoreType.DMA((total, 2)),
                pltpu.SemaphoreType.DMA((total, 2)),
                pltpu.SemaphoreType.DMA((total, 2)),
                pltpu.SemaphoreType.DMA((total, 2)),
            ],
            compiler_params=pltpu.CompilerParams(collective_id=0, has_side_effects=True, vmem_limit_bytes=62 * 1024 * 1024),
            name="layers",
        )(x, filter_taps.reshape(-1), wt, bias)
        return pl.pallas_call(
            unpack_kernel,
            grid=(vols, nq),
            in_specs=[pl.BlockSpec((1, 1, 512, 256), lambda v, p: (v, p, 0, 0))],
            out_specs=pl.BlockSpec((1, chans, h, ext, ext), lambda v, p: (v, 0, p, 0, 0)),
            out_shape=jax.ShapeDtypeStruct(x.shape, BF16),
            name="unpack",
        )(dense)

    return jax.shard_map(local, mesh=mesh, in_specs=(spec, P(), P(), P()), out_specs=spec, check_vma=False)
```

```python
import functools
import math

import jax
import jax.numpy as jnp
from jax import lax
from jax.experimental import pallas as pl
from jax.experimental.pallas import tpu as pltpu
from jax.sharding import PartitionSpec as P

MESH = pl.DeviceIdType.MESH
F32 = jnp.float32
BF16 = jnp.bfloat16
LAG_B = 3
LAG_C = 7


def dot(a, b):
    return jnp.dot(a, b, preferred_element_type=F32)


def iota2(shape, dim):
    return lax.broadcasted_iota(jnp.int32, shape, dim)


def kernel(cfg, x_hbm, taps_hbm, weight_hbm, bias_hbm, out_ref, taps, weight, bias, stage, vb, u1, u2, jsend, jlo, jhi, ksend, klo, khi,
           mi, mj, mjh, mk, mkh, mw, ms, bcol, arg_sem, in_sem, xs_sem, xr_sem, js_sem, jr_sem, ks_sem, kr_sem):
    layers, vols, nq, chans, ext, h, ktaps, ny, nz = cfg
    per_layer = vols * nq
    total = layers * per_layer
    px, py, pz = lax.axis_index("px"), lax.axis_index("py"), lax.axis_index("pz")
    mate = 1 - px
    y_lo, y_hi, z_lo, z_hi = py > 0, py < ny - 1, pz > 0, pz < nz - 1

    def place(q):
        return px * q + (1 - px) * (nq - 1 - q)

    def index(n):
        return n // per_layer, (n // nq) % vols, n % nq

    def in_copy(c):
        v, q = c // nq, c % nq
        return pltpu.make_async_copy(x_hbm.at[v, :, pl.ds(place(q) * h, h)], stage.at[c], in_sem.at[c])

    def x_copy(l, v):
        src = px * 1 + (1 - px) * nq
        dst = px * (nq + 1)
        return pltpu.make_async_remote_copy(vb.at[l, v, src], vb.at[l, v, dst], xs_sem.at[l, v], xr_sem.at[l, v],
                                            device_id={"px": mate}, device_id_type=MESH)

    def j_copies(n):
        return (
            (y_hi, y_lo, pltpu.make_async_remote_copy(jsend.at[n, 1], jlo.at[n], js_sem.at[n, 1], jr_sem.at[n, 0],
                                                      device_id={"py": py + 1}, device_id_type=MESH)),
            (y_lo, y_hi, pltpu.make_async_remote_copy(jsend.at[n, 0], jhi.at[n], js_sem.at[n, 0], jr_sem.at[n, 1],
                                                      device_id={"py": py - 1}, device_id_type=MESH)),
        )

    def k_copies(n):
        return (
            (z_hi, z_lo, pltpu.make_async_remote_copy(ksend.at[n, 1], klo.at[n], ks_sem.at[n, 1], kr_sem.at[n, 0],
                                                      device_id={"pz": pz + 1}, device_id_type=MESH)),
            (z_lo, z_hi, pltpu.make_async_remote_copy(ksend.at[n, 0], khi.at[n], ks_sem.at[n, 0], kr_sem.at[n, 1],
                                                      device_id={"pz": pz - 1}, device_id_type=MESH)),
        )

    lanes = iota2((ext, 256), 1)
    rows = iota2((ext, 256), 0)
    lane_i, lane_k = lanes // ext, lanes % ext

    def banded(layer, axis, diff):
        acc = jnp.zeros(diff.shape, F32)
        for t in range(ktaps):
            acc = jnp.where(diff == t, taps[layer, axis, t], acc)
        return acc

    def build_i(layer):
        vals = banded(layer, 0, iota2((3 * h, 256), 0) - iota2((3 * h, 256), 1) // ext)
        for i_in in range(3 * h):
            full = jnp.broadcast_to(vals[i_in:i_in + 1, :], (ext, 256))
            mi[layer, pl.ds(i_in * ext, ext), :] = jnp.where(lane_k == rows, full, 0.0).astype(BF16)

    def build_pack():
        dirn, hh, i8, kk = lanes // 128, (lanes // 64) % 2, (lanes // h) % 8, lanes % h
        for q in range(2):
            for g in range(8):
                hit = (hh == q) & (i8 == g) & (rows == kk + (ext - h) * dirn)
                ms[q, pl.ds(g * ext, ext), :] = jnp.where(hit, 1.0, 0.0).astype(BF16)

    def build_j(layer):
        tj = banded(layer, 1, lane_k - rows + h)
        l2, r2 = lanes[:, :128], rows[:, :128]
        d2, c2, jj = l2 // 64, (l2 // h) % 8, l2 % h
        tjh = banded(layer, 1, jj + d2 * (ext + h) - r2)
        for g in range(8):
            mj[layer, pl.ds(g * ext, ext), :] = jnp.where(lane_i == g, tj, 0.0).astype(BF16)
            mjh[layer, pl.ds(g * ext, ext), :] = jnp.where(c2 == g, tjh, 0.0).astype(BF16)

    def build_k(layer):
        tk = banded(layer, 2, rows - lane_k + h)
        for g in range(8):
            mk[layer, pl.ds(g * ext, ext), :] = jnp.where(lane_i == g, tk, 0.0).astype(BF16)
        l3, r3 = lanes[:16, :], rows[:16, :]
        zero = jnp.zeros((64, 256), BF16)
        for d in range(2):
            tkh = banded(layer, 2, r3 % h + d * (ext + h) - l3 % ext)
            for half in range(2):
                mkh[layer, 1 - half, pl.ds(d * 128 + half * 64, 64), :] = zero
                for g in range(0, 8, 2):
                    part = jnp.where(l3 // ext == g + r3 // h, tkh, 0.0).astype(BF16)
                    mkh[layer, half, pl.ds(d * 128 + half * 64 + g * h, 16), :] = part

    def build_mix(layer):
        e_rows = jnp.where(iota2((256, 16), 0) // 16 == iota2((256, 16), 1), 1.0, 0.0).astype(BF16)
        e_cols = jnp.where(iota2((16, 256), 1) // 16 == iota2((16, 256), 0), 1.0, 0.0).astype(BF16)
        tall = lax.dot_general(e_rows, weight[layer], (((1,), (1,)), ((), ())), preferred_element_type=F32)
        wide = dot(tall.astype(BF16), e_cols)
        mw[layer] = jnp.where(iota2((256, 256), 0) % 16 == iota2((256, 256), 1) % 16, wide, 0.0).astype(BF16)
        for d in range(chans):
            bcol[layer, pl.ds(d * 16, 16), :] = jnp.full((16, 128), bias[layer, d], F32)

    def convert(c):
        v, q = c // nq, c % nq
        in_copy(c).wait()
        parts = [stage[c, :, a].reshape(chans * ext, ext) for a in range(h)]
        vb[0, v, place(q) + 1] = jnp.concatenate(parts, axis=1)

    def when(cond, do):
        if isinstance(cond, bool):
            if cond:
                do()
        else:
            pl.when(cond)(do)

    def wait_x(n):
        l, v, q = index(n)
        when(q == 0, lambda: x_copy(l, v).wait_recv())

    def wait_all(copies):
        for _, here, copy in copies:
            pl.when(here)(copy.wait_recv)

    def start_all(copies):
        for there, _, copy in copies:
            pl.when(there)(copy.start)

    def compute_b(n):
        l, v, q = index(n)
        n_lo = jnp.where(y_lo, n, total)
        n_hi = jnp.where(y_hi, n, total)
        packed = None
        for half in range(2):
            main = u1[n % 4, pl.ds(half * 256, 256), :]
            halo = jnp.concatenate([jlo[n_lo, pl.ds(half * 64, 64), :], jhi[n_hi, pl.ds(half * 64, 64), :]], axis=0)
            acc = (dot(mj[l], main) + dot(mjh[l], halo)).astype(BF16)
            u2[n % 4, pl.ds(half * 256, 256), :] = acc
            term = dot(acc, ms[half])
            packed = term if packed is None else packed + term
        packed = packed.astype(BF16)
        ksend[n, 0] = packed[:, :128]
        ksend[n, 1] = packed[:, 128:]

    def compute_a(n):
        l, v, q = index(n)
        s = place(q) + 1
        acc = dot(vb[l, v, s - 1], mi[l, 0:256]) + dot(vb[l, v, s], mi[l, 256:512]) + dot(vb[l, v, s + 1], mi[l, 512:768])
        u1[n % 4] = acc.astype(BF16)
        cut = acc.reshape(chans, ext // h, h, 256)
        jsend[n, 0] = cut[:, 0].reshape(chans * h, 256).astype(BF16)
        jsend[n, 1] = cut[:, ext // h - 1].reshape(chans * h, 256).astype(BF16)

    def compute_c(n, store):
        l, v, q = index(n)
        n_lo = jnp.where(z_lo, n, total)
        n_hi = jnp.where(z_hi, n, total)
        halo = jnp.concatenate([klo[n_lo], khi[n_hi]], axis=1)
        u3 = []
        for half in range(2):
            acc = dot(u2[n % 4, pl.ds(half * 256, 256), :], mk[l]) + dot(halo, mkh[l, half])
            u3.append(acc.astype(BF16).reshape(8, 2, 16, 256))
        s = place(q) + 1
        b128 = bcol[l]
        shift = jnp.concatenate([b128, b128], axis=1)
        old = vb[l, v, s].reshape(chans, 2, 16, 256)
        new = []
        for jh in range(2):
            rhs = jnp.concatenate([u3[0][:, jh].reshape(128, 256), u3[1][:, jh].reshape(128, 256)], axis=0)
            z = dot(mw[l], rhs) + shift
            inner = z * (math.sqrt(2.0 / math.pi) + (0.044715 * math.sqrt(2.0 / math.pi)) * (z * z))
            half_z = 0.5 * z
            act = half_z + half_z * jnp.tanh(inner)
            res = old[:, jh].reshape(256, 256).astype(F32) + act
            new.append(res.astype(BF16).reshape(chans, 1, 16, 256))
        store(n, jnp.concatenate(new, axis=1).reshape(512, 256))

    def store_state(n, result):
        l, v, q = index(n)
        vb[l + 1, v, place(q) + 1] = result

    def store_out(n, result):
        l, v, q = index(n)
        out_ref[v, place(q)] = result

    def tick(a, b, c, last):
        if c is not None:
            wait_all(k_copies(c))
            compute_c(c, store_out if last else store_state)
            l, v, q = index(c)
            if not last:
                when(q == 0, lambda: x_copy(l + 1, v).start())
        if b is not None:
            wait_all(j_copies(b))
        if a is not None:
            wait_x(a)
        if b is not None:
            compute_b(b)
        if a is not None:
            compute_a(a)
        if b is not None:
            start_all(k_copies(b))
        if a is not None:
            start_all(j_copies(a))

    arg_copies = [pltpu.make_async_copy(taps_hbm, taps, arg_sem.at[0]),
                  pltpu.make_async_copy(weight_hbm, weight, arg_sem.at[1]),
                  pltpu.make_async_copy(bias_hbm, bias, arg_sem.at[2])]
    for copy in arg_copies:
        copy.start()
    for c in range(3):
        in_copy(c).start()
    barrier = pltpu.get_barrier_semaphore()
    pl.semaphore_signal(barrier, inc=1, device_id={"px": mate}, device_id_type=MESH)
    for cond, name, other in ((y_lo, "py", py - 1), (y_hi, "py", py + 1), (z_lo, "pz", pz - 1), (z_hi, "pz", pz + 1)):
        @pl.when(cond)
        def _(name=name, other=other):
            pl.semaphore_signal(barrier, inc=1, device_id={name: other}, device_id_type=MESH)

    for copy in arg_copies:
        copy.wait()
    build_i(0)
    edge_slot = px * (nq + 1)
    big_zero = jnp.zeros((512, 256), BF16)
    for l in range(layers):
        for v in range(vols):
            vb[l, v, edge_slot] = big_zero
    jlo[total] = jnp.zeros((128, 256), BF16)
    jhi[total] = jnp.zeros((128, 256), BF16)
    klo[total] = jnp.zeros((256, 128), BF16)
    khi[total] = jnp.zeros((256, 128), BF16)

    convert(0)
    n_wait = 1 + y_lo.astype(jnp.int32) + y_hi.astype(jnp.int32) + z_lo.astype(jnp.int32) + z_hi.astype(jnp.int32)
    pl.semaphore_wait(barrier, n_wait)
    x_copy(0, 0).start()
    for c in range(3, per_layer):
        in_copy(c).start()
    convert(1)

    for t in range(LAG_C):
        tick(t, t - LAG_B if t >= LAG_B else None, None, False)
        if t + 2 < per_layer:
            convert(t + 2)
            if (t + 2) % nq == 0:
                x_copy(0, (t + 2) // nq).start()
        if t == 0:
            build_j(0)
            build_pack()
        elif t == 1:
            build_k(0)
        elif t == 2:
            build_mix(0)
        elif t == 3:
            for l in range(1, layers):
                build_i(l)
        elif t == 4:
            for l in range(1, layers):
                build_j(l)
        elif t == 5:
            for l in range(1, layers):
                build_k(l)
                build_mix(l)

    split = per_layer * (layers - 1)

    def steady(t, _):
        tick(t, t - LAG_B, t - LAG_C, False)
        return 0

    lax.fori_loop(LAG_C, split + LAG_C, steady, 0)
    for t in range(split + LAG_C, total + LAG_C):
        tick(t if t < total else None, t - LAG_B if t < total + LAG_B else None, t - LAG_C, True)

    def drain(n, _):
        for there, _, copy in j_copies(n) + k_copies(n):
            pl.when(there)(copy.wait_send)
        return 0

    lax.fori_loop(0, total, drain, 0)
    for l in range(layers):
        for v in range(vols):
            x_copy(l, v).wait_send()


def unpack_kernel(nq, dense, o_hbm, stage, out_sem):
    vols, _, rows, width = dense.shape
    chans, h, ext = stage.shape[1:4]
    count = vols * nq
    outs = [pltpu.make_async_copy(stage.at[c], o_hbm.at[c // nq, :, pl.ds((c % nq) * h, h)], out_sem.at[c]) for c in range(count)]
    for c in range(count):
        for group in range(width // 128):
            block = dense[c // nq, c % nq, :, group * 128:(group + 1) * 128]
            for a in range(128 // ext):
                moved = block if a == 0 else pltpu.roll(block, 128 - ext * a, 1)
                stage[c, :, group * (128 // ext) + a] = moved[:, :ext].reshape(chans, ext, ext)
        outs[c].start()
    for copy in outs:
        copy.wait()


def solution(mesh):
    ny, nz = mesh.shape["py"], mesh.shape["pz"]
    spec = P("dp", None, "px", "py", "pz")

    def local(x, filter_taps, mix_weight, mix_bias):
        vols, chans, ext = x.shape[0], x.shape[1], x.shape[2]
        layers, ktaps = filter_taps.shape[0], filter_taps.shape[2]
        h = (ktaps - 1) // 2
        nq = ext // h
        total = layers * vols * nq
        cfg = (layers, vols, nq, chans, ext, h, ktaps, ny, nz)
        dense = pl.pallas_call(
            functools.partial(kernel, cfg),
            out_shape=jax.ShapeDtypeStruct((vols, nq, 512, 256), BF16),
            in_specs=[pl.BlockSpec(memory_space=pltpu.HBM)] * 4,
            out_specs=pl.BlockSpec(memory_space=pltpu.VMEM),
            scratch_shapes=[
                pltpu.SMEM(filter_taps.shape, F32),
                pltpu.VMEM(mix_weight.shape, BF16),
                pltpu.SMEM(mix_bias.shape, F32),
                pltpu.VMEM((vols * nq, chans, h, ext, ext), BF16),
                pltpu.VMEM((layers, vols, nq + 2, 512, 256), BF16),
                pltpu.VMEM((4, 512, 256), BF16),
                pltpu.VMEM((4, 512, 256), BF16),
                pltpu.VMEM((total, 2, 128, 256), BF16),
                pltpu.VMEM((total + 1, 128, 256), BF16),
                pltpu.VMEM((total + 1, 128, 256), BF16),
                pltpu.VMEM((total, 2, 256, 128), BF16),
                pltpu.VMEM((total + 1, 256, 128), BF16),
                pltpu.VMEM((total + 1, 256, 128), BF16),
                pltpu.VMEM((layers, 768, 256), BF16),
                pltpu.VMEM((layers, 256, 256), BF16),
                pltpu.VMEM((layers, 256, 128), BF16),
                pltpu.VMEM((layers, 256, 256), BF16),
                pltpu.VMEM((layers, 2, 256, 256), BF16),
                pltpu.VMEM((layers, 256, 256), BF16),
                pltpu.VMEM((2, 256, 256), BF16),
                pltpu.VMEM((layers, 256, 128), F32),
                pltpu.SemaphoreType.DMA((3,)),
                pltpu.SemaphoreType.DMA((vols * nq,)),
                pltpu.SemaphoreType.DMA((layers, vols)),
                pltpu.SemaphoreType.DMA((layers, vols)),
                pltpu.SemaphoreType.DMA((total, 2)),
                pltpu.SemaphoreType.DMA((total, 2)),
                pltpu.SemaphoreType.DMA((total, 2)),
                pltpu.SemaphoreType.DMA((total, 2)),
            ],
            compiler_params=pltpu.CompilerParams(collective_id=0, has_side_effects=True, vmem_limit_bytes=50 * 1024 * 1024),
            name="layers",
        )(x, filter_taps, mix_weight, mix_bias)
        return pl.pallas_call(
            functools.partial(unpack_kernel, nq),
            in_specs=[pl.BlockSpec(memory_space=pltpu.VMEM)],
            out_specs=pl.BlockSpec(memory_space=pl.ANY),
            out_shape=jax.ShapeDtypeStruct(x.shape, BF16),
            scratch_shapes=[
                pltpu.VMEM((vols * nq, chans, h, ext, ext), BF16),
                pltpu.SemaphoreType.DMA((vols * nq,)),
            ],
            compiler_params=pltpu.CompilerParams(vmem_limit_bytes=32 * 1024 * 1024),
            name="unpack",
        )(dense)

    return jax.shard_map(local, mesh=mesh, in_specs=(spec, P(), P(), P()), out_specs=spec, check_vma=False)
```

```python
import functools
import math

import jax
import jax.numpy as jnp
from jax import lax
from jax.experimental import pallas as pl
from jax.experimental.pallas import tpu as pltpu
from jax.sharding import PartitionSpec as P

MESH = pl.DeviceIdType.MESH
F32 = jnp.float32
BF16 = jnp.bfloat16
LAG_B = 3
LAG_C = 7


def dot(a, b):
    return jnp.dot(a, b, preferred_element_type=F32)


def iota2(shape, dim):
    return lax.broadcasted_iota(jnp.int32, shape, dim)


def kernel(cfg, x_hbm, taps_hbm, weight_hbm, bias_hbm, out_ref, taps, weight, bias, stage, vb, u1, u2, jsend, jlo, jhi, ksend, klo, khi,
           mi, mj, mjh, mk, mkh, mw, ms, bcol, arg_sem, in_sem, xs_sem, xr_sem, js_sem, jr_sem, ks_sem, kr_sem):
    layers, vols, nq, chans, ext, h, ktaps, ny, nz = cfg
    per_layer = vols * nq
    total = layers * per_layer
    px, py, pz = lax.axis_index("px"), lax.axis_index("py"), lax.axis_index("pz")
    mate = 1 - px
    y_lo, y_hi, z_lo, z_hi = py > 0, py < ny - 1, pz > 0, pz < nz - 1

    def place(q):
        return px * q + (1 - px) * (nq - 1 - q)

    def index(n):
        return n // per_layer, (n // nq) % vols, n % nq

    def in_copy(c):
        v, q = c // nq, c % nq
        return pltpu.make_async_copy(x_hbm.at[v, :, pl.ds(place(q) * h, h)], stage.at[c], in_sem.at[c])

    def x_copy(l, v):
        src = px * 1 + (1 - px) * nq
        dst = px * (nq + 1)
        return pltpu.make_async_remote_copy(vb.at[l, v, src], vb.at[l, v, dst], xs_sem.at[l, v], xr_sem.at[l, v],
                                            device_id={"px": mate}, device_id_type=MESH)

    def j_copies(n):
        return (
            (y_hi, y_lo, pltpu.make_async_remote_copy(jsend.at[n, 1], jlo.at[n], js_sem.at[n, 1], jr_sem.at[n, 0],
                                                      device_id={"py": py + 1}, device_id_type=MESH)),
            (y_lo, y_hi, pltpu.make_async_remote_copy(jsend.at[n, 0], jhi.at[n], js_sem.at[n, 0], jr_sem.at[n, 1],
                                                      device_id={"py": py - 1}, device_id_type=MESH)),
        )

    def k_copies(n):
        return (
            (z_hi, z_lo, pltpu.make_async_remote_copy(ksend.at[n, 1], klo.at[n], ks_sem.at[n, 1], kr_sem.at[n, 0],
                                                      device_id={"pz": pz + 1}, device_id_type=MESH)),
            (z_lo, z_hi, pltpu.make_async_remote_copy(ksend.at[n, 0], khi.at[n], ks_sem.at[n, 0], kr_sem.at[n, 1],
                                                      device_id={"pz": pz - 1}, device_id_type=MESH)),
        )

    lanes = iota2((ext, 256), 1)
    rows = iota2((ext, 256), 0)
    lane_i, lane_k = lanes // ext, lanes % ext

    def banded(layer, axis, diff):
        acc = jnp.zeros(diff.shape, F32)
        for t in range(ktaps):
            acc = jnp.where(diff == t, taps[layer, axis, t], acc)
        return acc

    def build_i(layer):
        vals = banded(layer, 0, iota2((3 * h, 256), 0) - iota2((3 * h, 256), 1) // ext)
        for i_in in range(3 * h):
            full = jnp.broadcast_to(vals[i_in:i_in + 1, :], (ext, 256))
            mi[layer, pl.ds(i_in * ext, ext), :] = jnp.where(lane_k == rows, full, 0.0).astype(BF16)

    def build_pack():
        dirn, hh, i8, kk = lanes // 128, (lanes // 64) % 2, (lanes // h) % 8, lanes % h
        for q in range(2):
            for g in range(8):
                hit = (hh == q) & (i8 == g) & (rows == kk + (ext - h) * dirn)
                ms[q, pl.ds(g * ext, ext), :] = jnp.where(hit, 1.0, 0.0).astype(BF16)

    def build_j(layer):
        tj = banded(layer, 1, lane_k - rows + h)
        l2, r2 = lanes[:, :128], rows[:, :128]
        d2, c2, jj = l2 // 64, (l2 // h) % 8, l2 % h
        tjh = banded(layer, 1, jj + d2 * (ext + h) - r2)
        for g in range(8):
            mj[layer, pl.ds(g * ext, ext), :] = jnp.where(lane_i == g, tj, 0.0).astype(BF16)
            mjh[layer, pl.ds(g * ext, ext), :] = jnp.where(c2 == g, tjh, 0.0).astype(BF16)

    def build_k(layer):
        tk = banded(layer, 2, rows - lane_k + h)
        for g in range(8):
            mk[layer, pl.ds(g * ext, ext), :] = jnp.where(lane_i == g, tk, 0.0).astype(BF16)
        l3, r3 = lanes[:16, :], rows[:16, :]
        zero = jnp.zeros((64, 256), BF16)
        for d in range(2):
            tkh = banded(layer, 2, r3 % h + d * (ext + h) - l3 % ext)
            for half in range(2):
                mkh[layer, 1 - half, pl.ds(d * 128 + half * 64, 64), :] = zero
                for g in range(0, 8, 2):
                    part = jnp.where(l3 // ext == g + r3 // h, tkh, 0.0).astype(BF16)
                    mkh[layer, half, pl.ds(d * 128 + half * 64 + g * h, 16), :] = part

    def build_mix(layer):
        e_rows = jnp.where(iota2((256, 16), 0) // 16 == iota2((256, 16), 1), 1.0, 0.0).astype(BF16)
        e_cols = jnp.where(iota2((16, 256), 1) // 16 == iota2((16, 256), 0), 1.0, 0.0).astype(BF16)
        tall = lax.dot_general(e_rows, weight[layer], (((1,), (1,)), ((), ())), preferred_element_type=F32)
        wide = dot(tall.astype(BF16), e_cols)
        mw[layer] = jnp.where(iota2((256, 256), 0) % 16 == iota2((256, 256), 1) % 16, wide, 0.0).astype(BF16)
        for d in range(chans):
            bcol[layer, pl.ds(d * 16, 16), :] = jnp.full((16, 128), bias[layer, d], F32)

    def convert(c):
        v, q = c // nq, c % nq
        in_copy(c).wait()
        parts = [stage[c, :, a].reshape(chans * ext, ext) for a in range(h)]
        vb[0, v, place(q) + 1] = jnp.concatenate(parts, axis=1)

    def when(cond, do):
        if isinstance(cond, bool):
            if cond:
                do()
        else:
            pl.when(cond)(do)

    def wait_x(n):
        l, v, q = index(n)
        when(q == 0, lambda: x_copy(l, v).wait_recv())

    def wait_all(copies):
        for _, here, copy in copies:
            pl.when(here)(copy.wait_recv)

    def start_all(copies):
        for there, _, copy in copies:
            pl.when(there)(copy.start)

    def compute_b(n):
        l, v, q = index(n)
        n_lo = jnp.where(y_lo, n, total)
        n_hi = jnp.where(y_hi, n, total)
        packed = None
        for half in range(2):
            main = u1[n % 4, pl.ds(half * 256, 256), :]
            halo = jnp.concatenate([jlo[n_lo, pl.ds(half * 64, 64), :], jhi[n_hi, pl.ds(half * 64, 64), :]], axis=0)
            acc = (dot(mj[l], main) + dot(mjh[l], halo)).astype(BF16)
            u2[n % 4, pl.ds(half * 256, 256), :] = acc
            term = dot(acc, ms[half])
            packed = term if packed is None else packed + term
        packed = packed.astype(BF16)
        ksend[n, 0] = packed[:, :128]
        ksend[n, 1] = packed[:, 128:]

    def compute_a(n):
        l, v, q = index(n)
        s = place(q) + 1
        acc = dot(vb[l, v, s - 1], mi[l, 0:256]) + dot(vb[l, v, s], mi[l, 256:512]) + dot(vb[l, v, s + 1], mi[l, 512:768])
        u1[n % 4] = acc.astype(BF16)
        cut = acc.reshape(chans, ext // h, h, 256)
        jsend[n, 0] = cut[:, 0].reshape(chans * h, 256).astype(BF16)
        jsend[n, 1] = cut[:, ext // h - 1].reshape(chans * h, 256).astype(BF16)

    def compute_c(n, store):
        l, v, q = index(n)
        n_lo = jnp.where(z_lo, n, total)
        n_hi = jnp.where(z_hi, n, total)
        halo = jnp.concatenate([klo[n_lo], khi[n_hi]], axis=1)
        u3 = []
        for half in range(2):
            acc = dot(u2[n % 4, pl.ds(half * 256, 256), :], mk[l]) + dot(halo, mkh[l, half])
            u3.append(acc.astype(BF16).reshape(8, 2, 16, 256))
        s = place(q) + 1
        b128 = bcol[l]
        shift = jnp.concatenate([b128, b128], axis=1)
        old = vb[l, v, s].reshape(chans, 2, 16, 256)
        new = []
        for jh in range(2):
            rhs = jnp.concatenate([u3[0][:, jh].reshape(128, 256), u3[1][:, jh].reshape(128, 256)], axis=0)
            z = dot(mw[l], rhs) + shift
            inner = z * (math.sqrt(2.0 / math.pi) + (0.044715 * math.sqrt(2.0 / math.pi)) * (z * z))
            half_z = 0.5 * z
            act = half_z + half_z * jnp.tanh(inner)
            res = old[:, jh].reshape(256, 256).astype(F32) + act
            new.append(res.astype(BF16).reshape(chans, 1, 16, 256))
        store(n, jnp.concatenate(new, axis=1).reshape(512, 256))

    def store_state(n, result):
        l, v, q = index(n)
        vb[l + 1, v, place(q) + 1] = result

    def store_out(n, result):
        l, v, q = index(n)
        out_ref[v, place(q)] = result

    def tick(a, b, c, last):
        if c is not None:
            wait_all(k_copies(c))
            compute_c(c, store_out if last else store_state)
            l, v, q = index(c)
            if not last:
                when(q == 0, lambda: x_copy(l + 1, v).start())
        if b is not None:
            wait_all(j_copies(b))
        if a is not None:
            wait_x(a)
        if b is not None:
            compute_b(b)
        if a is not None:
            compute_a(a)
        if b is not None:
            start_all(k_copies(b))
        if a is not None:
            start_all(j_copies(a))

    arg_copies = [pltpu.make_async_copy(taps_hbm, taps, arg_sem.at[0]),
                  pltpu.make_async_copy(weight_hbm, weight, arg_sem.at[1]),
                  pltpu.make_async_copy(bias_hbm, bias, arg_sem.at[2])]
    for copy in arg_copies:
        copy.start()
    for c in range(3):
        in_copy(c).start()
    barrier = pltpu.get_barrier_semaphore()
    pl.semaphore_signal(barrier, inc=1, device_id={"px": mate}, device_id_type=MESH)
    for cond, name, other in ((y_lo, "py", py - 1), (y_hi, "py", py + 1), (z_lo, "pz", pz - 1), (z_hi, "pz", pz + 1)):
        @pl.when(cond)
        def _(name=name, other=other):
            pl.semaphore_signal(barrier, inc=1, device_id={name: other}, device_id_type=MESH)

    for copy in arg_copies:
        copy.wait()
    build_i(0)
    edge_slot = px * (nq + 1)
    big_zero = jnp.zeros((512, 256), BF16)
    for l in range(layers):
        for v in range(vols):
            vb[l, v, edge_slot] = big_zero
    jlo[total] = jnp.zeros((128, 256), BF16)
    jhi[total] = jnp.zeros((128, 256), BF16)
    klo[total] = jnp.zeros((256, 128), BF16)
    khi[total] = jnp.zeros((256, 128), BF16)

    convert(0)
    n_wait = 1 + y_lo.astype(jnp.int32) + y_hi.astype(jnp.int32) + z_lo.astype(jnp.int32) + z_hi.astype(jnp.int32)
    pl.semaphore_wait(barrier, n_wait)
    x_copy(0, 0).start()
    for c in range(3, per_layer):
        in_copy(c).start()
    convert(1)

    for t in range(LAG_C):
        tick(t, t - LAG_B if t >= LAG_B else None, None, False)
        if t + 2 < per_layer:
            convert(t + 2)
            if (t + 2) % nq == 0:
                x_copy(0, (t + 2) // nq).start()
        if t == 0:
            build_j(0)
            build_pack()
        elif t == 1:
            build_k(0)
        elif t == 2:
            build_mix(0)
        elif t == 3:
            for l in range(1, layers):
                build_i(l)
        elif t == 4:
            for l in range(1, layers):
                build_j(l)
        elif t == 5:
            for l in range(1, layers):
                build_k(l)
                build_mix(l)

    split = per_layer * (layers - 1)

    def steady(t, _):
        tick(t, t - LAG_B, t - LAG_C, False)
        return 0

    lax.fori_loop(LAG_C, split + LAG_C, steady, 0)
    for t in range(split + LAG_C, total + LAG_C):
        tick(t if t < total else None, t - LAG_B if t < total + LAG_B else None, t - LAG_C, True)

    def drain(n, _):
        for there, _, copy in j_copies(n) + k_copies(n):
            pl.when(there)(copy.wait_send)
        return 0

    lax.fori_loop(0, total, drain, 0)
    for l in range(layers):
        for v in range(vols):
            x_copy(l, v).wait_send()


def unpack_kernel(nq, dense, o_hbm, stage, out_sem):
    vols, _, rows, width = dense.shape
    chans, h, ext = stage.shape[1:4]
    count = vols * nq
    outs = [pltpu.make_async_copy(stage.at[c], o_hbm.at[c // nq, :, pl.ds((c % nq) * h, h)], out_sem.at[c]) for c in range(count)]
    for c in range(count):
        for group in range(width // 128):
            block = dense[c // nq, c % nq, :, group * 128:(group + 1) * 128]
            for a in range(128 // ext):
                moved = block if a == 0 else pltpu.roll(block, 128 - ext * a, 1)
                stage[c, :, group * (128 // ext) + a] = moved[:, :ext].reshape(chans, ext, ext)
        outs[c].start()
    for copy in outs:
        copy.wait()


def solution(mesh):
    ny, nz = mesh.shape["py"], mesh.shape["pz"]
    spec = P("dp", None, "px", "py", "pz")

    def local(x, filter_taps, mix_weight, mix_bias):
        vols, chans, ext = x.shape[0], x.shape[1], x.shape[2]
        layers, ktaps = filter_taps.shape[0], filter_taps.shape[2]
        h = (ktaps - 1) // 2
        nq = ext // h
        total = layers * vols * nq
        cfg = (layers, vols, nq, chans, ext, h, ktaps, ny, nz)
        dense = pl.pallas_call(
            functools.partial(kernel, cfg),
            out_shape=jax.ShapeDtypeStruct((vols, nq, 512, 256), BF16),
            in_specs=[pl.BlockSpec(memory_space=pltpu.HBM)] * 4,
            out_specs=pl.BlockSpec(memory_space=pltpu.VMEM),
            scratch_shapes=[
                pltpu.SMEM(filter_taps.shape, F32),
                pltpu.VMEM(mix_weight.shape, BF16),
                pltpu.SMEM(mix_bias.shape, F32),
                pltpu.VMEM((vols * nq, chans, h, ext, ext), BF16),
                pltpu.VMEM((layers, vols, nq + 2, 512, 256), BF16),
                pltpu.VMEM((4, 512, 256), BF16),
                pltpu.VMEM((4, 512, 256), BF16),
                pltpu.VMEM((total, 2, 128, 256), BF16),
                pltpu.VMEM((total + 1, 128, 256), BF16),
                pltpu.VMEM((total + 1, 128, 256), BF16),
                pltpu.VMEM((total, 2, 256, 128), BF16),
                pltpu.VMEM((total + 1, 256, 128), BF16),
                pltpu.VMEM((total + 1, 256, 128), BF16),
                pltpu.VMEM((layers, 768, 256), BF16),
                pltpu.VMEM((layers, 256, 256), BF16),
                pltpu.VMEM((layers, 256, 128), BF16),
                pltpu.VMEM((layers, 256, 256), BF16),
                pltpu.VMEM((layers, 2, 256, 256), BF16),
                pltpu.VMEM((layers, 256, 256), BF16),
                pltpu.VMEM((2, 256, 256), BF16),
                pltpu.VMEM((layers, 256, 128), F32),
                pltpu.SemaphoreType.DMA((3,)),
                pltpu.SemaphoreType.DMA((vols * nq,)),
                pltpu.SemaphoreType.DMA((layers, vols)),
                pltpu.SemaphoreType.DMA((layers, vols)),
                pltpu.SemaphoreType.DMA((total, 2)),
                pltpu.SemaphoreType.DMA((total, 2)),
                pltpu.SemaphoreType.DMA((total, 2)),
                pltpu.SemaphoreType.DMA((total, 2)),
            ],
            compiler_params=pltpu.CompilerParams(collective_id=0, has_side_effects=True, vmem_limit_bytes=50 * 1024 * 1024),
            name="layers",
        )(x, *(pltpu.with_memory_space_constraint(a, pltpu.HBM) for a in (filter_taps, mix_weight, mix_bias)))
        return pl.pallas_call(
            functools.partial(unpack_kernel, nq),
            in_specs=[pl.BlockSpec(memory_space=pltpu.VMEM)],
            out_specs=pl.BlockSpec(memory_space=pl.ANY),
            out_shape=jax.ShapeDtypeStruct(x.shape, BF16),
            scratch_shapes=[
                pltpu.VMEM((vols * nq, chans, h, ext, ext), BF16),
                pltpu.SemaphoreType.DMA((vols * nq,)),
            ],
            compiler_params=pltpu.CompilerParams(vmem_limit_bytes=32 * 1024 * 1024),
            name="unpack",
        )(dense)

    return jax.shard_map(local, mesh=mesh, in_specs=(spec, P(), P(), P()), out_specs=spec, check_vma=False)
```

```python
import functools
import math

import jax
import jax.numpy as jnp
from jax import lax
from jax.experimental import pallas as pl
from jax.experimental.pallas import tpu as pltpu
from jax.sharding import PartitionSpec as P

MESH = pl.DeviceIdType.MESH
F32 = jnp.float32
BF16 = jnp.bfloat16
LAG_B = 3
LAG_C = 7


def dot(a, b):
    return jnp.dot(a, b, preferred_element_type=F32)


def iota2(shape, dim):
    return lax.broadcasted_iota(jnp.int32, shape, dim)


def kernel(cfg, x_hbm, taps_hbm, weight_hbm, bias_hbm, out_ref, taps, weight, bias, stage, vb, u1, u2, jsend, jlo, jhi, ksend, klo, khi,
           mi, mj, mjh, mk, mkh, mw, ms, bcol, arg_sem, in_sem, xs_sem, xr_sem, js_sem, jr_sem, ks_sem, kr_sem):
    layers, vols, nq, chans, ext, h, ktaps, ny, nz = cfg
    per_layer = vols * nq
    total = layers * per_layer
    px, py, pz = lax.axis_index("px"), lax.axis_index("py"), lax.axis_index("pz")
    mate = 1 - px
    y_lo, y_hi, z_lo, z_hi = py > 0, py < ny - 1, pz > 0, pz < nz - 1

    def place(q):
        return px * q + (1 - px) * (nq - 1 - q)

    def index(n):
        return n // per_layer, (n // nq) % vols, n % nq

    def in_copy(c):
        v, q = c // nq, c % nq
        return pltpu.make_async_copy(x_hbm.at[v, :, pl.ds(place(q) * h, h)], stage.at[c], in_sem.at[c])

    def x_copy(l, v):
        src = px * 1 + (1 - px) * nq
        dst = px * (nq + 1)
        return pltpu.make_async_remote_copy(vb.at[l, v, src], vb.at[l, v, dst], xs_sem.at[l, v], xr_sem.at[l, v],
                                            device_id={"px": mate}, device_id_type=MESH)

    def j_copies(n):
        return (
            (y_hi, y_lo, pltpu.make_async_remote_copy(jsend.at[n, 1], jlo.at[n], js_sem.at[n, 1], jr_sem.at[n, 0],
                                                      device_id={"py": py + 1}, device_id_type=MESH)),
            (y_lo, y_hi, pltpu.make_async_remote_copy(jsend.at[n, 0], jhi.at[n], js_sem.at[n, 0], jr_sem.at[n, 1],
                                                      device_id={"py": py - 1}, device_id_type=MESH)),
        )

    def k_copies(n):
        return (
            (z_hi, z_lo, pltpu.make_async_remote_copy(ksend.at[n, 1], klo.at[n], ks_sem.at[n, 1], kr_sem.at[n, 0],
                                                      device_id={"pz": pz + 1}, device_id_type=MESH)),
            (z_lo, z_hi, pltpu.make_async_remote_copy(ksend.at[n, 0], khi.at[n], ks_sem.at[n, 0], kr_sem.at[n, 1],
                                                      device_id={"pz": pz - 1}, device_id_type=MESH)),
        )

    lanes = iota2((ext, 256), 1)
    rows = iota2((ext, 256), 0)
    lane_i, lane_k = lanes // ext, lanes % ext

    def banded(layer, axis, diff):
        acc = jnp.zeros(diff.shape, F32)
        for t in range(ktaps):
            acc = jnp.where(diff == t, taps[layer, axis, t], acc)
        return acc

    def build_i(layer):
        vals = banded(layer, 0, iota2((3 * h, 256), 0) - iota2((3 * h, 256), 1) // ext)
        for i_in in range(3 * h):
            full = jnp.broadcast_to(vals[i_in:i_in + 1, :], (ext, 256))
            mi[layer, pl.ds(i_in * ext, ext), :] = jnp.where(lane_k == rows, full, 0.0).astype(BF16)

    def build_pack():
        dirn, hh, i8, kk = lanes // 128, (lanes // 64) % 2, (lanes // h) % 8, lanes % h
        for q in range(2):
            for g in range(8):
                hit = (hh == q) & (i8 == g) & (rows == kk + (ext - h) * dirn)
                ms[q, pl.ds(g * ext, ext), :] = jnp.where(hit, 1.0, 0.0).astype(BF16)

    def build_j(layer):
        tj = banded(layer, 1, lane_k - rows + h)
        l2, r2 = lanes[:, :128], rows[:, :128]
        d2, c2, jj = l2 // 64, (l2 // h) % 8, l2 % h
        tjh = banded(layer, 1, jj + d2 * (ext + h) - r2)
        for g in range(8):
            mj[layer, pl.ds(g * ext, ext), :] = jnp.where(lane_i == g, tj, 0.0).astype(BF16)
            mjh[layer, pl.ds(g * ext, ext), :] = jnp.where(c2 == g, tjh, 0.0).astype(BF16)

    def build_k(layer):
        tk = banded(layer, 2, rows - lane_k + h)
        for g in range(8):
            mk[layer, pl.ds(g * ext, ext), :] = jnp.where(lane_i == g, tk, 0.0).astype(BF16)
        l3, r3 = lanes[:16, :], rows[:16, :]
        zero = jnp.zeros((64, 256), BF16)
        for d in range(2):
            tkh = banded(layer, 2, r3 % h + d * (ext + h) - l3 % ext)
            for half in range(2):
                mkh[layer, 1 - half, pl.ds(d * 128 + half * 64, 64), :] = zero
                for g in range(0, 8, 2):
                    part = jnp.where(l3 // ext == g + r3 // h, tkh, 0.0).astype(BF16)
                    mkh[layer, half, pl.ds(d * 128 + half * 64 + g * h, 16), :] = part

    def build_mix(layer):
        e_rows = jnp.where(iota2((256, 16), 0) // 16 == iota2((256, 16), 1), 1.0, 0.0).astype(BF16)
        e_cols = jnp.where(iota2((16, 256), 1) // 16 == iota2((16, 256), 0), 1.0, 0.0).astype(BF16)
        tall = lax.dot_general(e_rows, weight[layer], (((1,), (1,)), ((), ())), preferred_element_type=F32)
        wide = dot(tall.astype(BF16), e_cols)
        mw[layer] = jnp.where(iota2((256, 256), 0) % 16 == iota2((256, 256), 1) % 16, wide, 0.0).astype(BF16)
        for d in range(chans):
            bcol[layer, pl.ds(d * 16, 16), :] = jnp.full((16, 128), bias[layer, d], F32)

    def convert(c):
        v, q = c // nq, c % nq
        in_copy(c).wait()
        parts = [stage[c, :, a].reshape(chans * ext, ext) for a in range(h)]
        vb[0, v, place(q) + 1] = jnp.concatenate(parts, axis=1)

    def when(cond, do):
        if isinstance(cond, bool):
            if cond:
                do()
        else:
            pl.when(cond)(do)

    def wait_x(n):
        l, v, q = index(n)
        when(q == 0, lambda: x_copy(l, v).wait_recv())

    def wait_all(copies):
        for _, here, copy in copies:
            pl.when(here)(copy.wait_recv)

    def start_all(copies):
        for there, _, copy in copies:
            pl.when(there)(copy.start)

    def compute_b(n):
        l, v, q = index(n)
        n_lo = jnp.where(y_lo, n, total)
        n_hi = jnp.where(y_hi, n, total)
        packed = None
        for half in range(2):
            main = u1[n % 4, pl.ds(half * 256, 256), :]
            halo = jnp.concatenate([jlo[n_lo, pl.ds(half * 64, 64), :], jhi[n_hi, pl.ds(half * 64, 64), :]], axis=0)
            acc = (dot(mj[l], main) + dot(mjh[l], halo)).astype(BF16)
            u2[n % 4, pl.ds(half * 256, 256), :] = acc
            term = dot(acc, ms[half])
            packed = term if packed is None else packed + term
        packed = packed.astype(BF16)
        ksend[n, 0] = packed[:, :128]
        ksend[n, 1] = packed[:, 128:]

    def compute_a(n):
        l, v, q = index(n)
        s = place(q) + 1
        acc = dot(vb[l, v, s - 1], mi[l, 0:256]) + dot(vb[l, v, s], mi[l, 256:512]) + dot(vb[l, v, s + 1], mi[l, 512:768])
        u1[n % 4] = acc.astype(BF16)
        cut = acc.reshape(chans, ext // h, h, 256)
        jsend[n, 0] = cut[:, 0].reshape(chans * h, 256).astype(BF16)
        jsend[n, 1] = cut[:, ext // h - 1].reshape(chans * h, 256).astype(BF16)

    def compute_c(n, store):
        l, v, q = index(n)
        n_lo = jnp.where(z_lo, n, total)
        n_hi = jnp.where(z_hi, n, total)
        halo = jnp.concatenate([klo[n_lo], khi[n_hi]], axis=1)
        u3 = []
        for half in range(2):
            acc = dot(u2[n % 4, pl.ds(half * 256, 256), :], mk[l]) + dot(halo, mkh[l, half])
            u3.append(acc.astype(BF16).reshape(8, 2, 16, 256))
        s = place(q) + 1
        b128 = bcol[l]
        shift = jnp.concatenate([b128, b128], axis=1)
        old = vb[l, v, s].reshape(chans, 2, 16, 256)
        new = []
        for jh in range(2):
            rhs = jnp.concatenate([u3[0][:, jh].reshape(128, 256), u3[1][:, jh].reshape(128, 256)], axis=0)
            z = dot(mw[l], rhs) + shift
            inner = z * (math.sqrt(2.0 / math.pi) + (0.044715 * math.sqrt(2.0 / math.pi)) * (z * z))
            half_z = 0.5 * z
            act = half_z + half_z * jnp.tanh(inner)
            res = old[:, jh].reshape(256, 256).astype(F32) + act
            new.append(res.astype(BF16).reshape(chans, 1, 16, 256))
        store(n, jnp.concatenate(new, axis=1).reshape(512, 256))

    def store_state(n, result):
        l, v, q = index(n)
        vb[l + 1, v, place(q) + 1] = result

    def store_out(n, result):
        l, v, q = index(n)
        out_ref[v, place(q)] = result

    def tick(a, b, c, last):
        if c is not None:
            wait_all(k_copies(c))
            compute_c(c, store_out if last else store_state)
            l, v, q = index(c)
            if not last:
                when(q == 0, lambda: x_copy(l + 1, v).start())
        if b is not None:
            wait_all(j_copies(b))
        if a is not None:
            wait_x(a)
        if b is not None:
            compute_b(b)
        if a is not None:
            compute_a(a)
        if a is not None:
            start_all(j_copies(a))
        if b is not None:
            start_all(k_copies(b))

    arg_copies = [pltpu.make_async_copy(taps_hbm, taps, arg_sem.at[0]),
                  pltpu.make_async_copy(weight_hbm, weight, arg_sem.at[1]),
                  pltpu.make_async_copy(bias_hbm, bias, arg_sem.at[2])]
    in_copy(0).start()
    for copy in arg_copies:
        copy.start()
    barrier = pltpu.get_barrier_semaphore()
    pl.semaphore_signal(barrier, inc=1, device_id={"px": mate}, device_id_type=MESH)
    for cond, name, other in ((y_lo, "py", py - 1), (y_hi, "py", py + 1), (z_lo, "pz", pz - 1), (z_hi, "pz", pz + 1)):
        @pl.when(cond)
        def _(name=name, other=other):
            pl.semaphore_signal(barrier, inc=1, device_id={name: other}, device_id_type=MESH)

    edge_slot = px * (nq + 1)
    big_zero = jnp.zeros((512, 256), BF16)
    for l in range(layers):
        for v in range(vols):
            vb[l, v, edge_slot] = big_zero
    jlo[total] = jnp.zeros((128, 256), BF16)
    jhi[total] = jnp.zeros((128, 256), BF16)
    klo[total] = jnp.zeros((256, 128), BF16)
    khi[total] = jnp.zeros((256, 128), BF16)

    in_copy(1).start()
    convert(0)
    n_wait = 1 + y_lo.astype(jnp.int32) + y_hi.astype(jnp.int32) + z_lo.astype(jnp.int32) + z_hi.astype(jnp.int32)
    pl.semaphore_wait(barrier, n_wait)
    x_copy(0, 0).start()
    for c in range(2, per_layer):
        in_copy(c).start()
    for copy in arg_copies:
        copy.wait()
    build_i(0)
    convert(1)

    for t in range(LAG_C):
        tick(t, t - LAG_B if t >= LAG_B else None, None, False)
        if t + 2 < per_layer:
            convert(t + 2)
            if (t + 2) % nq == 0:
                x_copy(0, (t + 2) // nq).start()
        if t == 1:
            build_j(0)
            build_pack()
        elif t == 2:
            build_k(0)
            build_mix(0)
        elif t == 3:
            for l in range(1, layers):
                build_i(l)
        elif t == 4:
            for l in range(1, layers):
                build_j(l)
        elif t == 5:
            for l in range(1, layers):
                build_k(l)
        elif t == 6:
            for l in range(1, layers):
                build_mix(l)

    split = per_layer * (layers - 1)

    def steady(t, _):
        tick(t, t - LAG_B, t - LAG_C, False)
        return 0

    lax.fori_loop(LAG_C, split + LAG_C, steady, 0)
    for t in range(split + LAG_C, total + LAG_C):
        tick(t if t < total else None, t - LAG_B if t < total + LAG_B else None, t - LAG_C, True)

    def drain(n, _):
        for there, _, copy in j_copies(n) + k_copies(n):
            pl.when(there)(copy.wait_send)
        return 0

    lax.fori_loop(0, total, drain, 0)
    for l in range(layers):
        for v in range(vols):
            x_copy(l, v).wait_send()


def unpack_kernel(nq, dense, o_hbm, stage, out_sem):
    vols, _, rows, width = dense.shape
    chans, h, ext = stage.shape[1:4]
    groups, span = width // 128, 128 // ext
    outs = []
    for c in range(vols * nq):
        for group in range(groups):
            block = dense[c // nq, c % nq, :, group * 128:(group + 1) * 128]
            for a in range(span):
                moved = block if a == 0 else pltpu.roll(block, 128 - ext * a, 1)
                stage[c, :, group * span + a] = moved[:, :ext].reshape(chans, ext, ext)
            outs.append(pltpu.make_async_copy(stage.at[c, :, pl.ds(group * span, span)],
                                              o_hbm.at[c // nq, :, pl.ds((c % nq) * h + group * span, span)], out_sem.at[c, group]))
            outs[-1].start()
    for copy in outs:
        copy.wait()


def solution(mesh):
    ny, nz = mesh.shape["py"], mesh.shape["pz"]
    spec = P("dp", None, "px", "py", "pz")

    def local(x, filter_taps, mix_weight, mix_bias):
        vols, chans, ext = x.shape[0], x.shape[1], x.shape[2]
        layers, ktaps = filter_taps.shape[0], filter_taps.shape[2]
        h = (ktaps - 1) // 2
        nq = ext // h
        total = layers * vols * nq
        cfg = (layers, vols, nq, chans, ext, h, ktaps, ny, nz)
        dense = pl.pallas_call(
            functools.partial(kernel, cfg),
            out_shape=jax.ShapeDtypeStruct((vols, nq, 512, 256), BF16),
            in_specs=[pl.BlockSpec(memory_space=pltpu.HBM)] * 4,
            out_specs=pl.BlockSpec(memory_space=pltpu.VMEM),
            scratch_shapes=[
                pltpu.SMEM(filter_taps.shape, F32),
                pltpu.VMEM(mix_weight.shape, BF16),
                pltpu.SMEM(mix_bias.shape, F32),
                pltpu.VMEM((vols * nq, chans, h, ext, ext), BF16),
                pltpu.VMEM((layers, vols, nq + 2, 512, 256), BF16),
                pltpu.VMEM((4, 512, 256), BF16),
                pltpu.VMEM((4, 512, 256), BF16),
                pltpu.VMEM((total, 2, 128, 256), BF16),
                pltpu.VMEM((total + 1, 128, 256), BF16),
                pltpu.VMEM((total + 1, 128, 256), BF16),
                pltpu.VMEM((total, 2, 256, 128), BF16),
                pltpu.VMEM((total + 1, 256, 128), BF16),
                pltpu.VMEM((total + 1, 256, 128), BF16),
                pltpu.VMEM((layers, 768, 256), BF16),
                pltpu.VMEM((layers, 256, 256), BF16),
                pltpu.VMEM((layers, 256, 128), BF16),
                pltpu.VMEM((layers, 256, 256), BF16),
                pltpu.VMEM((layers, 2, 256, 256), BF16),
                pltpu.VMEM((layers, 256, 256), BF16),
                pltpu.VMEM((2, 256, 256), BF16),
                pltpu.VMEM((layers, 256, 128), F32),
                pltpu.SemaphoreType.DMA((3,)),
                pltpu.SemaphoreType.DMA((vols * nq,)),
                pltpu.SemaphoreType.DMA((layers, vols)),
                pltpu.SemaphoreType.DMA((layers, vols)),
                pltpu.SemaphoreType.DMA((total, 2)),
                pltpu.SemaphoreType.DMA((total, 2)),
                pltpu.SemaphoreType.DMA((total, 2)),
                pltpu.SemaphoreType.DMA((total, 2)),
            ],
            compiler_params=pltpu.CompilerParams(collective_id=0, has_side_effects=True, vmem_limit_bytes=50 * 1024 * 1024),
            name="layers",
        )(x, *(pltpu.with_memory_space_constraint(a, pltpu.HBM) for a in (filter_taps, mix_weight, mix_bias)))
        return pl.pallas_call(
            functools.partial(unpack_kernel, nq),
            in_specs=[pl.BlockSpec(memory_space=pltpu.VMEM)],
            out_specs=pl.BlockSpec(memory_space=pl.ANY),
            out_shape=jax.ShapeDtypeStruct(x.shape, BF16),
            scratch_shapes=[
                pltpu.VMEM((vols * nq, chans, h, ext, ext), BF16),
                pltpu.SemaphoreType.DMA((vols * nq, 2)),
            ],
            compiler_params=pltpu.CompilerParams(vmem_limit_bytes=32 * 1024 * 1024),
            name="unpack",
        )(dense)

    return jax.shard_map(local, mesh=mesh, in_specs=(spec, P(), P(), P()), out_specs=spec, check_vma=False)
```

```python
import functools
import math

import jax
import jax.numpy as jnp
from jax import lax
from jax.experimental import pallas as pl
from jax.experimental.pallas import tpu as pltpu
from jax.sharding import PartitionSpec as P

MESH = pl.DeviceIdType.MESH
F32 = jnp.float32
BF16 = jnp.bfloat16
LAG_B = 3
LAG_C = 7


def dot(a, b):
    return jnp.dot(a, b, preferred_element_type=F32)


def iota2(shape, dim):
    return lax.broadcasted_iota(jnp.int32, shape, dim)


def kernel(cfg, x_hbm, taps_hbm, weight_hbm, bias_hbm, out_ref, taps, weight, bias, stage, vb, u1, u2, jsend, jlo, jhi, ksend, klo, khi,
           mi, mj, mjh, mk, mkh, mw, ms, bcol, arg_sem, in_sem, xs_sem, xr_sem, js_sem, jr_sem, ks_sem, kr_sem):
    layers, vols, nq, chans, ext, h, ktaps, ny, nz = cfg
    per_layer = vols * nq
    total = layers * per_layer
    px, py, pz = lax.axis_index("px"), lax.axis_index("py"), lax.axis_index("pz")
    mate = 1 - px
    y_lo, y_hi, z_lo, z_hi = py > 0, py < ny - 1, pz > 0, pz < nz - 1

    def place(q):
        return px * q + (1 - px) * (nq - 1 - q)

    def index(n):
        return n // per_layer, (n // nq) % vols, n % nq

    def in_copy(c):
        v, q = c // nq, c % nq
        return pltpu.make_async_copy(x_hbm.at[v, :, pl.ds(place(q) * h, h)], stage.at[c], in_sem.at[c])

    def x_copy(l, v):
        src = px * 1 + (1 - px) * nq
        dst = px * (nq + 1)
        return pltpu.make_async_remote_copy(vb.at[l, v, src], vb.at[l, v, dst], xs_sem.at[l, v], xr_sem.at[l, v],
                                            device_id={"px": mate}, device_id_type=MESH)

    def j_copies(n):
        return (
            (y_hi, y_lo, pltpu.make_async_remote_copy(jsend.at[n, 1], jlo.at[n], js_sem.at[n, 1], jr_sem.at[n, 0],
                                                      device_id={"py": py + 1}, device_id_type=MESH)),
            (y_lo, y_hi, pltpu.make_async_remote_copy(jsend.at[n, 0], jhi.at[n], js_sem.at[n, 0], jr_sem.at[n, 1],
                                                      device_id={"py": py - 1}, device_id_type=MESH)),
        )

    def k_copies(n):
        return (
            (z_hi, z_lo, pltpu.make_async_remote_copy(ksend.at[n, 1], klo.at[n], ks_sem.at[n, 1], kr_sem.at[n, 0],
                                                      device_id={"pz": pz + 1}, device_id_type=MESH)),
            (z_lo, z_hi, pltpu.make_async_remote_copy(ksend.at[n, 0], khi.at[n], ks_sem.at[n, 0], kr_sem.at[n, 1],
                                                      device_id={"pz": pz - 1}, device_id_type=MESH)),
        )

    lanes = iota2((ext, 256), 1)
    rows = iota2((ext, 256), 0)
    lane_i, lane_k = lanes // ext, lanes % ext

    def banded(layer, axis, diff):
        acc = jnp.zeros(diff.shape, F32)
        for t in range(ktaps):
            acc = jnp.where(diff == t, taps[layer, axis, t], acc)
        return acc

    def build_i(layer):
        vals = banded(layer, 0, iota2((3 * h, 256), 0) - iota2((3 * h, 256), 1) // ext)
        for i_in in range(3 * h):
            full = jnp.broadcast_to(vals[i_in:i_in + 1, :], (ext, 256))
            mi[layer, pl.ds(i_in * ext, ext), :] = jnp.where(lane_k == rows, full, 0.0).astype(BF16)

    def build_pack():
        dirn, hh, i8, kk = lanes // 128, (lanes // 64) % 2, (lanes // h) % 8, lanes % h
        for q in range(2):
            for g in range(8):
                hit = (hh == q) & (i8 == g) & (rows == kk + (ext - h) * dirn)
                ms[q, pl.ds(g * ext, ext), :] = jnp.where(hit, 1.0, 0.0).astype(BF16)

    def build_j(layer):
        tj = banded(layer, 1, lane_k - rows + h)
        l2, r2 = lanes[:, :128], rows[:, :128]
        d2, c2, jj = l2 // 64, (l2 // h) % 8, l2 % h
        tjh = banded(layer, 1, jj + d2 * (ext + h) - r2)
        for g in range(8):
            mj[layer, pl.ds(g * ext, ext), :] = jnp.where(lane_i == g, tj, 0.0).astype(BF16)
            mjh[layer, pl.ds(g * ext, ext), :] = jnp.where(c2 == g, tjh, 0.0).astype(BF16)

    def build_k(layer):
        tk = banded(layer, 2, rows - lane_k + h)
        for g in range(8):
            mk[layer, pl.ds(g * ext, ext), :] = jnp.where(lane_i == g, tk, 0.0).astype(BF16)
        l3, r3 = lanes[:16, :], rows[:16, :]
        zero = jnp.zeros((64, 256), BF16)
        for d in range(2):
            tkh = banded(layer, 2, r3 % h + d * (ext + h) - l3 % ext)
            for half in range(2):
                mkh[layer, 1 - half, pl.ds(d * 128 + half * 64, 64), :] = zero
                for g in range(0, 8, 2):
                    part = jnp.where(l3 // ext == g + r3 // h, tkh, 0.0).astype(BF16)
                    mkh[layer, half, pl.ds(d * 128 + half * 64 + g * h, 16), :] = part

    def build_mix(layer):
        e_rows = jnp.where(iota2((256, 16), 0) // 16 == iota2((256, 16), 1), 1.0, 0.0).astype(BF16)
        e_cols = jnp.where(iota2((16, 256), 1) // 16 == iota2((16, 256), 0), 1.0, 0.0).astype(BF16)
        tall = lax.dot_general(e_rows, weight[layer], (((1,), (1,)), ((), ())), preferred_element_type=F32)
        wide = dot(tall.astype(BF16), e_cols)
        mw[layer] = jnp.where(iota2((256, 256), 0) % 16 == iota2((256, 256), 1) % 16, wide, 0.0).astype(BF16)
        for d in range(chans):
            bcol[layer, pl.ds(d * 16, 16), :] = jnp.full((16, 128), bias[layer, d], F32)

    def convert(c):
        v, q = c // nq, c % nq
        in_copy(c).wait()
        parts = [stage[c, :, a].reshape(chans * ext, ext) for a in range(h)]
        vb[0, v, place(q) + 1] = jnp.concatenate(parts, axis=1)

    def when(cond, do):
        if isinstance(cond, bool):
            if cond:
                do()
        else:
            pl.when(cond)(do)

    def wait_x(n):
        l, v, q = index(n)
        when(q == 0, lambda: x_copy(l, v).wait_recv())

    def wait_all(copies):
        for _, here, copy in copies:
            pl.when(here)(copy.wait_recv)

    def start_all(copies):
        for there, _, copy in copies:
            pl.when(there)(copy.start)

    def compute_b(n):
        l, v, q = index(n)
        n_lo = jnp.where(y_lo, n, total)
        n_hi = jnp.where(y_hi, n, total)
        packed = None
        for half in range(2):
            main = u1[n % 4, pl.ds(half * 256, 256), :]
            halo = jnp.concatenate([jlo[n_lo, pl.ds(half * 64, 64), :], jhi[n_hi, pl.ds(half * 64, 64), :]], axis=0)
            acc = (dot(mj[l], main) + dot(mjh[l], halo)).astype(BF16)
            u2[n % 4, pl.ds(half * 256, 256), :] = acc
            term = dot(acc, ms[half])
            packed = term if packed is None else packed + term
        packed = packed.astype(BF16)
        ksend[n, 0] = packed[:, :128]
        ksend[n, 1] = packed[:, 128:]

    def compute_a(n):
        l, v, q = index(n)
        s = place(q) + 1
        acc = dot(vb[l, v, s - 1], mi[l, 0:256]) + dot(vb[l, v, s], mi[l, 256:512]) + dot(vb[l, v, s + 1], mi[l, 512:768])
        u1[n % 4] = acc.astype(BF16)
        cut = acc.reshape(chans, ext // h, h, 256)
        jsend[n, 0] = cut[:, 0].reshape(chans * h, 256).astype(BF16)
        jsend[n, 1] = cut[:, ext // h - 1].reshape(chans * h, 256).astype(BF16)

    def compute_c(n, store):
        l, v, q = index(n)
        n_lo = jnp.where(z_lo, n, total)
        n_hi = jnp.where(z_hi, n, total)
        halo = jnp.concatenate([klo[n_lo], khi[n_hi]], axis=1)
        u3 = []
        for half in range(2):
            acc = dot(u2[n % 4, pl.ds(half * 256, 256), :], mk[l]) + dot(halo, mkh[l, half])
            u3.append(acc.astype(BF16).reshape(8, 2, 16, 256))
        s = place(q) + 1
        b128 = bcol[l]
        shift = jnp.concatenate([b128, b128], axis=1)
        old = vb[l, v, s].reshape(chans, 2, 16, 256)
        new = []
        for jh in range(2):
            rhs = jnp.concatenate([u3[0][:, jh].reshape(128, 256), u3[1][:, jh].reshape(128, 256)], axis=0)
            z = dot(mw[l], rhs) + shift
            inner = z * (math.sqrt(2.0 / math.pi) + (0.044715 * math.sqrt(2.0 / math.pi)) * (z * z))
            half_z = 0.5 * z
            act = half_z + half_z * jnp.tanh(inner)
            res = old[:, jh].reshape(256, 256).astype(F32) + act
            new.append(res.astype(BF16).reshape(chans, 1, 16, 256))
        store(n, jnp.concatenate(new, axis=1).reshape(512, 256))

    def store_state(n, result):
        l, v, q = index(n)
        vb[l + 1, v, place(q) + 1] = result

    def store_out(n, result):
        l, v, q = index(n)
        out_ref[v, place(q)] = result

    def tick(a, b, c, last):
        if c is not None:
            wait_all(k_copies(c))
            compute_c(c, store_out if last else store_state)
            l, v, q = index(c)
            if not last:
                when(q == 0, lambda: x_copy(l + 1, v).start())
        if b is not None:
            wait_all(j_copies(b))
        if a is not None:
            wait_x(a)
        if b is not None:
            compute_b(b)
        if a is not None:
            compute_a(a)
        if a is not None:
            start_all(j_copies(a))
        if b is not None:
            start_all(k_copies(b))

    arg_copies = [pltpu.make_async_copy(taps_hbm, taps, arg_sem.at[0]),
                  pltpu.make_async_copy(weight_hbm, weight, arg_sem.at[1]),
                  pltpu.make_async_copy(bias_hbm, bias, arg_sem.at[2])]
    in_copy(0).start()
    for copy in arg_copies:
        copy.start()
    barrier = pltpu.get_barrier_semaphore()
    pl.semaphore_signal(barrier, inc=1, device_id={"px": mate}, device_id_type=MESH)
    for cond, name, other in ((y_lo, "py", py - 1), (y_hi, "py", py + 1), (z_lo, "pz", pz - 1), (z_hi, "pz", pz + 1)):
        @pl.when(cond)
        def _(name=name, other=other):
            pl.semaphore_signal(barrier, inc=1, device_id={name: other}, device_id_type=MESH)

    edge_slot = px * (nq + 1)
    big_zero = jnp.zeros((512, 256), BF16)
    for l in range(layers):
        for v in range(vols):
            vb[l, v, edge_slot] = big_zero
    jlo[total] = jnp.zeros((128, 256), BF16)
    jhi[total] = jnp.zeros((128, 256), BF16)
    klo[total] = jnp.zeros((256, 128), BF16)
    khi[total] = jnp.zeros((256, 128), BF16)

    in_copy(1).start()
    convert(0)
    n_wait = 1 + y_lo.astype(jnp.int32) + y_hi.astype(jnp.int32) + z_lo.astype(jnp.int32) + z_hi.astype(jnp.int32)
    pl.semaphore_wait(barrier, n_wait)
    x_copy(0, 0).start()
    for c in range(2, per_layer):
        in_copy(c).start()
    for copy in arg_copies:
        copy.wait()
    build_i(0)
    convert(1)

    for t in range(LAG_C):
        tick(t, t - LAG_B if t >= LAG_B else None, None, False)
        if t + 2 < per_layer:
            convert(t + 2)
            if (t + 2) % nq == 0:
                x_copy(0, (t + 2) // nq).start()
        if t == 1:
            build_j(0)
            build_pack()
        elif t == 2:
            build_k(0)
            build_mix(0)
        elif t == 3:
            for l in range(1, layers):
                build_i(l)
        elif t == 4:
            for l in range(1, layers):
                build_j(l)
        elif t == 5:
            for l in range(1, layers):
                build_k(l)
        elif t == 6:
            for l in range(1, layers):
                build_mix(l)

    split = per_layer * (layers - 1)

    def steady(t, _):
        tick(t, t - LAG_B, t - LAG_C, False)
        return 0

    lax.fori_loop(LAG_C, split + LAG_C, steady, 0)
    def drain(n, _):
        for there, _, copy in j_copies(n) + k_copies(n):
            pl.when(there)(copy.wait_send)
        return 0

    for t in range(split + LAG_C, total + LAG_C):
        if t == total + LAG_C - 1:
            lax.fori_loop(0, total - 2, drain, 0)
            for l in range(layers):
                for v in range(vols):
                    x_copy(l, v).wait_send()
        tick(t if t < total else None, t - LAG_B if t < total + LAG_B else None, t - LAG_C, True)

    lax.fori_loop(total - 2, total, drain, 0)


def unpack_kernel(nq, dense, o_hbm, stage, out_sem):
    vols, _, rows, width = dense.shape
    chans, h, ext = stage.shape[1:4]
    groups, span = width // 128, 128 // ext
    outs = []
    for c in range(vols * nq):
        for group in range(groups):
            block = dense[c // nq, c % nq, :, group * 128:(group + 1) * 128]
            for a in range(span):
                moved = block if a == 0 else pltpu.roll(block, 128 - ext * a, 1)
                stage[c, :, group * span + a] = moved[:, :ext].reshape(chans, ext, ext)
            outs.append(pltpu.make_async_copy(stage.at[c, :, pl.ds(group * span, span)],
                                              o_hbm.at[c // nq, :, pl.ds((c % nq) * h + group * span, span)], out_sem.at[c, group]))
            outs[-1].start()
    for copy in outs:
        copy.wait()


def solution(mesh):
    ny, nz = mesh.shape["py"], mesh.shape["pz"]
    spec = P("dp", None, "px", "py", "pz")

    def local(x, filter_taps, mix_weight, mix_bias):
        vols, chans, ext = x.shape[0], x.shape[1], x.shape[2]
        layers, ktaps = filter_taps.shape[0], filter_taps.shape[2]
        h = (ktaps - 1) // 2
        nq = ext // h
        total = layers * vols * nq
        cfg = (layers, vols, nq, chans, ext, h, ktaps, ny, nz)
        dense = pl.pallas_call(
            functools.partial(kernel, cfg),
            out_shape=jax.ShapeDtypeStruct((vols, nq, 512, 256), BF16),
            in_specs=[pl.BlockSpec(memory_space=pltpu.HBM)] * 4,
            out_specs=pl.BlockSpec(memory_space=pltpu.VMEM),
            scratch_shapes=[
                pltpu.SMEM(filter_taps.shape, F32),
                pltpu.VMEM(mix_weight.shape, BF16),
                pltpu.SMEM(mix_bias.shape, F32),
                pltpu.VMEM((vols * nq, chans, h, ext, ext), BF16),
                pltpu.VMEM((layers, vols, nq + 2, 512, 256), BF16),
                pltpu.VMEM((4, 512, 256), BF16),
                pltpu.VMEM((4, 512, 256), BF16),
                pltpu.VMEM((total, 2, 128, 256), BF16),
                pltpu.VMEM((total + 1, 128, 256), BF16),
                pltpu.VMEM((total + 1, 128, 256), BF16),
                pltpu.VMEM((total, 2, 256, 128), BF16),
                pltpu.VMEM((total + 1, 256, 128), BF16),
                pltpu.VMEM((total + 1, 256, 128), BF16),
                pltpu.VMEM((layers, 768, 256), BF16),
                pltpu.VMEM((layers, 256, 256), BF16),
                pltpu.VMEM((layers, 256, 128), BF16),
                pltpu.VMEM((layers, 256, 256), BF16),
                pltpu.VMEM((layers, 2, 256, 256), BF16),
                pltpu.VMEM((layers, 256, 256), BF16),
                pltpu.VMEM((2, 256, 256), BF16),
                pltpu.VMEM((layers, 256, 128), F32),
                pltpu.SemaphoreType.DMA((3,)),
                pltpu.SemaphoreType.DMA((vols * nq,)),
                pltpu.SemaphoreType.DMA((layers, vols)),
                pltpu.SemaphoreType.DMA((layers, vols)),
                pltpu.SemaphoreType.DMA((total, 2)),
                pltpu.SemaphoreType.DMA((total, 2)),
                pltpu.SemaphoreType.DMA((total, 2)),
                pltpu.SemaphoreType.DMA((total, 2)),
            ],
            compiler_params=pltpu.CompilerParams(collective_id=0, has_side_effects=True, vmem_limit_bytes=50 * 1024 * 1024),
            name="layers",
        )(x, *(pltpu.with_memory_space_constraint(a, pltpu.HBM) for a in (filter_taps, mix_weight, mix_bias)))
        return pl.pallas_call(
            functools.partial(unpack_kernel, nq),
            in_specs=[pl.BlockSpec(memory_space=pltpu.VMEM)],
            out_specs=pl.BlockSpec(memory_space=pl.ANY),
            out_shape=jax.ShapeDtypeStruct(x.shape, BF16),
            scratch_shapes=[
                pltpu.VMEM((vols * nq, chans, h, ext, ext), BF16),
                pltpu.SemaphoreType.DMA((vols * nq, 2)),
            ],
            compiler_params=pltpu.CompilerParams(vmem_limit_bytes=32 * 1024 * 1024),
            name="unpack",
        )(dense)

    return jax.shard_map(local, mesh=mesh, in_specs=(spec, P(), P(), P()), out_specs=spec, check_vma=False)
```
